32 devices in a mesh: dp: 4 (over z), head: 8 (over y, x, core).
Axes of the slice: x: 2, y: 2, z: 4, core: 2. Of those that a mesh axis runs over, the one named last changes fastest.
Arguments:
- residual: float32 [96, 4096], P('dp', 'head'), parts along dimension 0, may hold values from -70 to 70
- norm_gain: float32 [4096], replicated, may hold values from 0.5 to 1.5
- w_query: bfloat16 [8, 256, 4096], P(None, 'head'), may hold values from -0.09375 to 0.09375
- w_key: bfloat16 [8, 256, 4096], P(None, 'head'), may hold values from -0.09375 to 0.09375
- w_value: bfloat16 [4096, 4096], P(None, 'head'), may hold values from -0.09375 to 0.09375
- w_gate: bfloat16 [4096, 4096], P(None, 'head'), may hold values from -0.09375 to 0.09375
- w_input: bfloat16 [8, 4096], replicated, may hold values from -0.09375 to 0.09375
- w_forget: bfloat16 [8, 4096], replicated, may hold values from -0.09375 to 0.09375
- b_input: float32 [8], replicated, may hold values from -2 to -0.5
- b_forget: float32 [8], replicated, may hold values from 0.5 to 4
- w_out: bfloat16 [4096, 4096], P('head'), may hold values from -0.125 to 0.125
- memory: bfloat16 [96, 8, 256, 512], P('dp', None, 'head'), parts along dimension 0, may hold values from -0.59765625 to 0.59765625
- normalizer: float32 [96, 8, 256], P('dp', None, 'head'), parts along dimension 0, may hold values from -0.6 to 0.6
- stabilizer: float32 [96, 8], P('dp'), parts along dimension 0, may hold values from -0.5 to 0.5
Outputs:
- res_out: float32 [96, 4096], P('dp', 'head'), parts along dimension 0
- mem_out: bfloat16 [96, 8, 256, 512], P('dp', None, 'head'), parts along dimension 0
- norm_out: float32 [96, 8, 256], P('dp', None, 'head'), parts along dimension 0
- stab_out: float32 [96, 8], P('dp'), parts along dimension 0
The draws below stay inside these ranges and needn't reach their ends.
There are 4 independent parts, one for each index of `dp`. The reference program is written for one: setup_inputs(seed, part) draws one part's arguments, and reference() takes and returns one part's arrays. A program takes and returns all parts, laid end to end along the dimension named above; an argument that names none is the same for every part. Nothing has to cross between parts.
All inputs are finite; a program needn't handle non-finite values.
Results may differ from the reference program's by a relative error of at most 0.0095.
Values may be sent and summed in bfloat16 or wider, within the bound.
A program may use at most 64 MiB of HBM per device.

```python
import math
import jax
import jax.numpy as jnp
from jax import lax

D = 4096
H = 8
DK = 256
DV = 512
B = 24


def draw_residual(key, part):
    key_base = jax.random.fold_in(key, 11)
    key_cols = jax.random.fold_in(key, 12)
    key_rows = jax.random.fold_in(key, 13)
    position = jnp.arange(D, dtype=jnp.float32) / D
    col_log = 0.5 * jnp.log(3.0) * position + jax.random.uniform(key_cols, (D,), jnp.float32, -1.15, 1.15)
    row_log = jax.random.uniform(key_rows, (B,), jnp.float32, -0.6, 0.6)
    base_vals = jax.random.truncated_normal(key_base, -4.0, 4.0, (B, D), jnp.float32)
    return base_vals * jnp.exp(row_log[:, None] + col_log[None, :])


def strengthened(result, own_key, source, target, shards_of, factor):
    owner, partner = [(jnp.arange(result.shape[dim]) // (result.shape[dim] // shards_of)).reshape([-1 if axis == dim else 1 for axis in range(result.ndim)]) for dim in (source, target)]
    chosen = jax.random.permutation(own_key, shards_of)[partner]
    strong = (owner == chosen) | (owner == (partner + shards_of // 2) % shards_of)
    return jnp.where(strong, factor * result, result)


def steps_of(rng, dims, pieces, low, high):
    level = 1.0
    for axis_at, parts in pieces:
        heights = jax.random.uniform(jax.random.fold_in(jax.random.fold_in(rng, 6), axis_at), (parts,), jnp.float32, low / len(pieces), high / len(pieces))
        level = level * jnp.repeat(jnp.exp(heights), dims[axis_at] // parts).reshape((-1,) + (1,) * (len(dims) - 1 - axis_at))
    return level


def bell_draw(rng, extent, deviation, bound, shards=(), kind=jnp.bfloat16):
    drawn = deviation * jax.random.normal(rng, extent, jnp.float32)
    if shards:
        drawn = drawn * steps_of(rng, extent, shards, -0.22, 0.18)
    return jnp.clip(drawn, -bound, bound).astype(kind)


def heavy_noise(key, extent, width, most, shards, heavy, kind=jnp.bfloat16):
    values = width * jax.random.normal(key, extent, jnp.float32)
    if shards:
        values = values * steps_of(key, extent, shards, -0.22, 0.18)
    return jnp.clip(strengthened(values, jax.random.fold_in(key, 3), *heavy), -most, most).astype(kind)


def setup_inputs(seed: int = 0, part: int = 0) -> dict:
    keys = jax.random.split(jax.random.key(seed), 15)
    part_keys = jax.random.split(jax.random.fold_in(keys[14], part), 15)
    residual = draw_residual(jax.random.fold_in(jax.random.fold_in(keys[14], part), 71), part)
    norm_gain = jnp.clip(1.0 + 0.1 * jax.random.normal(keys[1], (D,), jnp.float32), 0.5, 1.5)
    w_query = bell_draw(keys[2], (H, DK, D), D ** -0.5, 0.09375, ((1, 8),))
    w_key = bell_draw(keys[3], (H, DK, D), D ** -0.5, 0.09375, ((1, 8),))
    w_value = bell_draw(keys[4], (D, H * DV), D ** -0.5, 0.09375, ((1, 8),))
    w_gate = bell_draw(keys[5], (D, H * DV), D ** -0.5, 0.09375, ((1, 8),))
    w_input = bell_draw(keys[6], (H, D), D ** -0.5, 0.09375)
    w_forget = bell_draw(keys[7], (H, D), D ** -0.5, 0.09375)
    b_input = jnp.clip(jax.random.uniform(keys[8], (H,), jnp.float32, -2.0, -0.5), -2.0, -0.5)
    b_forget = jnp.clip(jax.random.uniform(keys[9], (H,), jnp.float32, 0.5, 4.0), 0.5, 4.0)
    w_out = heavy_noise(keys[10], (H * DV, D), (H * DV) ** -0.5, 0.125, ((0, 8),), (0, 1, 8, 2.0))
    memory = heavy_noise(part_keys[11], (B, H, DK, DV), 0.1, 0.59765625, ((2, 8),), (2, 3, 8, 2.0))
    normalizer = bell_draw(part_keys[12], (B, H, DK), 0.1, 0.6, ((2, 8),), jnp.float32)
    stabilizer = jnp.clip(jax.random.uniform(part_keys[13], (B, H), jnp.float32, -0.5, 0.5), -0.5, 0.5)
    return dict(residual=residual, norm_gain=norm_gain, w_query=w_query, w_key=w_key, w_value=w_value, w_gate=w_gate, w_input=w_input, w_forget=w_forget, b_input=b_input, b_forget=b_forget, w_out=w_out, memory=memory, normalizer=normalizer, stabilizer=stabilizer)


epsilon = 1e-06

def reference(residual, norm_gain, w_query, w_key, w_value, w_gate, w_input, w_forget, b_input, b_forget, w_out, memory, normalizer, stabilizer):
    mean_sq = lax.optimization_barrier(jnp.mean(residual * residual, axis=1, keepdims=True))
    x_norm = (residual * lax.rsqrt(mean_sq + epsilon) * norm_gain).astype(jnp.bfloat16)
    x_wide = x_norm.astype(jnp.float32)
    query_vec = jnp.einsum('bd,hkd->bhk', x_wide, w_query.astype(jnp.float32))
    key_vec = jnp.einsum('bd,hkd->bhk', x_wide, w_key.astype(jnp.float32)) / math.sqrt(DK)
    value_vec = jnp.dot(x_norm, w_value, preferred_element_type=jnp.float32).astype(jnp.bfloat16)
    input_pre = jnp.dot(x_norm, w_input.T, preferred_element_type=jnp.float32) + b_input
    forget_pre = jnp.dot(x_norm, w_forget.T, preferred_element_type=jnp.float32) + b_forget
    log_forget = jax.nn.log_sigmoid(forget_pre)
    stab_new = jnp.maximum(log_forget + stabilizer, input_pre)
    input_gate = jnp.exp(input_pre - stab_new)
    forget_gate = jnp.exp(log_forget + stabilizer - stab_new)
    batch_size = residual.shape[0]
    value_heads = value_vec.astype(jnp.float32).reshape(batch_size, H, DV)
    memory_full = forget_gate[:, :, None, None] * memory.astype(jnp.float32) + input_gate[:, :, None, None] * key_vec[:, :, :, None] * value_heads[:, :, None, :]
    norm_new = forget_gate[:, :, None] * normalizer + input_gate[:, :, None] * key_vec
    numerator = lax.optimization_barrier(jnp.sum(memory_full * query_vec[:, :, :, None], axis=2))
    denom_all = lax.optimization_barrier(jnp.sum(norm_new * query_vec, axis=2))
    readout = numerator / jnp.maximum(jnp.abs(denom_all), jnp.exp(-stab_new))[:, :, None]
    out_gate = jax.nn.sigmoid(jnp.dot(x_norm, w_gate, preferred_element_type=jnp.float32))
    hidden = (out_gate * readout.reshape(batch_size, H * DV)).astype(jnp.bfloat16)
    res_out = residual + jnp.dot(hidden, w_out, preferred_element_type=jnp.float32)
    return (res_out, memory_full.astype(jnp.bfloat16), norm_new, stab_new)
```

```python
import functools
import math

import jax
import jax.numpy as jnp
from jax import lax
from jax.experimental import pallas as pl
from jax.experimental.pallas import tpu as pltpu
from jax.sharding import PartitionSpec as P

GROUP = 8
LANES = 128
PIECES = 4
epsilon = 1e-06

NT = (((1,), (1,)), ((), ()))
NN = (((1,), (0,)), ((), ()))


def dot(a, b, dims=NN, precision=None):
    return lax.dot_general(a, b, dims, precision=precision, preferred_element_type=jnp.float32)


def kernel(
    n, batch, heads, rows, dv, width, key_scale,
    res_hbm, gain_hbm, wq_hbm, wk_hbm, wv_hbm, wg_hbm, wi_hbm, wf_hbm, bi_hbm, bf_hbm, wo_hbm, mem_hbm, nrm_hbm, stab_hbm,
    res_out, mem_out, nrm_out, stab_out,
    res, gain, wq, wk, wv, wg, wi, wf, bi, bf, wo, mem, nrm, stab,
    xs, sq, num_send, num_recv, den_send, den_recv, vals, out_send, out_recv,
    kt_ref, n_rows, num_tile, val_rows, f_rows, kcols,
    in_sem, mem_sem, x_send, x_recv, sq_send, sq_recv, num_ss, num_rs, den_ss, den_rs, val_ss, val_rs, out_ss, out_rs,
):
    me = lax.axis_index("head")
    groups = batch // GROUP
    hr = heads * rows
    share = n * width // heads
    barrier = pltpu.get_barrier_semaphore()

    def peer(d):
        other = me
        for k in range(n.bit_length() - 1):
            if d >> k & 1:
                other += (1 << k) * (1 - 2 * lax.rem(lax.div(me, 1 << k), 2))
        return other

    source = peer

    def other(k):
        return k + lax.div(k + n - me, n)

    far_first = sorted(range(1, n), key=lambda d: (-(d >> 1).bit_count(), d % 2))

    for d in far_first:
        pl.semaphore_signal(barrier, inc=1, device_id={"head": peer(d)}, device_id_type=pl.DeviceIdType.MESH)

    gain_part = gain_hbm.at[:, pl.ds(pl.multiple_of(me * width, width), width)]
    local = [
        (res_hbm, res), (gain_part, gain), (wq_hbm, wq), (wk_hbm, wk), (wi_hbm, wi), (wf_hbm, wf), (bi_hbm, bi), (bf_hbm, bf),
        (nrm_hbm, nrm), (stab_hbm, stab), (wv_hbm, wv), (wg_hbm, wg), (wo_hbm, wo),
    ]
    loads = [pltpu.make_async_copy(a, b, in_sem.at[i]) for i, (a, b) in enumerate(local)]
    (l_res, l_gain, l_wq, l_wk, l_wi, l_wf, l_bi, l_bf, l_nrm, l_stab, l_wv, l_wg, l_wo) = loads

    def mem_load(g):
        return pltpu.make_async_copy(
            mem_hbm.at[pl.ds(g * GROUP, GROUP)], mem.at[pl.ds(g * GROUP, GROUP)], mem_sem.at[g]
        )

    for copy in (l_res, l_gain, l_wq, l_wk):
        copy.start()
    for g in range(groups):
        mem_load(g).start()
    for copy in (l_wi, l_wf, l_bi, l_bf, l_nrm, l_stab, l_wv, l_wg, l_wo):
        copy.start()

    def remote(src, dst, ssem, rsem, target):
        return pltpu.make_async_remote_copy(
            src_ref=src, dst_ref=dst, send_sem=ssem, recv_sem=rsem,
            device_id={"head": target}, device_id_type=pl.DeviceIdType.MESH,
        )

    eye = lax.broadcasted_iota(jnp.int32, (batch, batch), 0) == lax.broadcasted_iota(jnp.int32, (batch, batch), 1)

    def to_row(col):
        return jnp.sum(jnp.where(eye, col, 0.0), axis=0, keepdims=True)

    def to_col(row):
        return jnp.sum(jnp.where(eye, row, 0.0), axis=1, keepdims=True)

    l_res.wait()
    l_gain.wait()
    own = res[...]
    xs[me] = (own * gain[...]).astype(jnp.bfloat16)
    sq[me] = jnp.zeros((1, LANES), jnp.float32)
    sq[me, :, 0:batch] = to_row(jnp.sum(own * own, axis=1, keepdims=True))
    den_send[...] = jnp.zeros_like(den_send)

    def x_copy(d, owner):
        return remote(xs.at[owner], xs.at[owner], x_send.at[d - 1], x_recv.at[d - 1], peer(d))

    def sq_copy(d, owner):
        return remote(sq.at[owner], sq.at[owner], sq_send.at[d - 1], sq_recv.at[d - 1], peer(d))

    def val_copy(d, owner):
        return remote(vals.at[owner], vals.at[owner], val_ss.at[d - 1], val_rs.at[d - 1], peer(d))

    def num_copy(d, g):
        return remote(num_send.at[peer(d), g], num_recv.at[d - 1, g], num_ss.at[d - 1, g], num_rs.at[d - 1, g], peer(d))

    def den_copy(d):
        head = lax.div(peer(d) * width, share)
        return remote(den_send.at[head], den_recv.at[d - 1], den_ss.at[d - 1], den_rs.at[d - 1], peer(d))

    def out_copy(k, owner, target):
        return remote(out_send.at[k], out_recv.at[owner], out_ss.at[k], out_rs.at[owner], target)

    pl.semaphore_wait(barrier, n - 1)
    for d in [1, 3, 5, 7, 2, 4, 6]:
        x_copy(d, me).start()
    for d in far_first:
        sq_copy(d, me).start()

    l_wq.wait()
    l_wk.wait()
    l_nrm.wait()
    q_t = jnp.zeros((hr, batch), jnp.float32)
    k_t = jnp.zeros((hr, batch), jnp.float32)
    for d in [0, 1, 3, 5, 2, 4, 7, 6]:
        owner = source(d)
        if d:
            with jax.named_scope(f"qk{d}_wait"):
                x_copy(d, owner).wait_recv()
        cols = pl.ds(pl.multiple_of(owner * width, width), width)
        block = xs[owner]
        q_t += dot(wq[:, cols], block, NT)
        k_t += dot(wk[:, cols], block, NT)
    kt_ref[...] = k_t
    q_raw = jnp.transpose(q_t)

    mine = lax.broadcasted_iota(jnp.int32, (heads, hr), 1) // rows == lax.broadcasted_iota(jnp.int32, (heads, hr), 0)

    def numerators(g):
        block_q = q_raw[g * GROUP : (g + 1) * GROUP, :]
        for j in range(GROUP):
            spread = jnp.where(mine, block_q[j : j + 1, :], 0.0)
            high = spread.astype(jnp.bfloat16)
            low = (spread - high.astype(jnp.float32)).astype(jnp.bfloat16)
            both = dot(jnp.concatenate([high, low], axis=0), mem[g * GROUP + j])
            num_tile[:, j, :] = both[:heads] + both[heads:]
        for p in range(n):
            head, col = p * width // dv, p * width % dv
            num_send[p, g] = num_tile[head, :, col : col + width].astype(jnp.bfloat16)

    def split_sum(product):
        high = product.astype(jnp.bfloat16)
        low = (product - high.astype(jnp.float32)).astype(jnp.bfloat16)
        return dot(ones, high, NT) + dot(ones, low, NT)

    ones = mine.astype(jnp.bfloat16)
    for g in range(groups):
        mem_load(g).wait()
        numerators(g)
        if g == groups - 1:
            k_raw = jnp.transpose(kt_ref[...])
            for h in range(heads):
                n_rows[:, h * rows : (h + 1) * rows] = nrm[:, h, :]
            nq = split_sum(n_rows[...] * q_raw)
            kq = split_sum(k_raw * q_raw)
            for h in range(heads):
                den_send[h, 0:1, 0:batch] = nq[h : h + 1]
                den_send[h, 1:2, 0:batch] = kq[h : h + 1]
        for d in far_first:
            num_copy(d, g).start()
    for d in far_first:
        den_copy(d).start()
    for d in far_first:
        sq_copy(d, source(d)).wait_recv()
    total = sq[0]
    for p in range(1, n):
        total += sq[p]
    s_row = lax.rsqrt(total[:, 0:batch] / (n * width) + epsilon)
    s_col = to_col(s_row)
    l_wv.wait()
    value = jnp.zeros((batch, width), jnp.float32)
    for p in range(n):
        value += dot(xs[p], wv[p * width : (p + 1) * width, :])
    value = (value * s_col).astype(jnp.bfloat16)
    vals[me] = value
    for d in far_first:
        val_copy(d, me).start()

    for copy in (l_wi, l_wf, l_bi, l_bf, l_stab):
        copy.wait()
    w_both = jnp.concatenate([wi[...], wf[...]], axis=0)
    pre = jnp.zeros((2 * heads, batch), jnp.float32)
    for p in range(n):
        pre += dot(w_both[:, p * width : (p + 1) * width], xs[p], NT)
    pre = pre * s_row
    eye_h = lax.broadcasted_iota(jnp.int32, (heads, heads), 0) == lax.broadcasted_iota(jnp.int32, (heads, heads), 1)
    bias_i = jnp.sum(jnp.where(eye_h, bi[...], 0.0), axis=1, keepdims=True)
    bias_f = jnp.sum(jnp.where(eye_h, bf[...], 0.0), axis=1, keepdims=True)
    input_pre = pre[:heads] + bias_i
    forget_pre = pre[heads:] + bias_f
    log_forget = jnp.minimum(forget_pre, 0.0) - jnp.log1p(jnp.exp(-jnp.abs(forget_pre)))
    carried = log_forget + stab[...]
    stab_new = jnp.maximum(carried, input_pre)
    stab_out[...] = stab_new
    i_gate = jnp.exp(input_pre - stab_new)
    f_gate = jnp.exp(carried - stab_new)

    key = k_raw * (s_col * key_scale)
    l_wg.wait()
    cuts = 2 if width % (2 * LANES) == 0 else 1
    half = width // cuts
    gates2 = [jnp.zeros((batch, half), jnp.float32) for _ in range(cuts)]
    for p in range(n):
        for e in range(cuts):
            gates2[e] += dot(xs[p], wg[p * width : (p + 1) * width, e * half : (e + 1) * half])
    gate = jnp.concatenate(gates2, axis=1)
    gate = jax.nn.sigmoid(gate * s_col)

    key_t = kt_ref[...] * (s_row * key_scale)
    for h in range(heads):
        at = slice(h * rows, (h + 1) * rows)
        ik = key_t[at, :] * i_gate[h : h + 1, :]
        f_rows[h] = jnp.broadcast_to(to_col(f_gate[h : h + 1, :]), (batch, LANES)).reshape(groups, GROUP, LANES)
        for g in range(groups):
            kcols[g, at, :] = ik[:, g * GROUP : (g + 1) * GROUP]
    for h in range(heads):
        nrm_out[:, h, :] = to_col(f_gate[h : h + 1, :]) * nrm[:, h, :] + (
            to_col(i_gate[h : h + 1, :]) * key[:, h * rows : (h + 1) * rows]
        )

    my_head = lax.div(me * width, share)
    picked = lax.broadcasted_iota(jnp.int32, (heads, batch), 0) == my_head

    def pick(table):
        return jnp.sum(jnp.where(picked, table, 0.0), axis=0, keepdims=True)

    den = den_send[my_head]
    for d in range(1, n):
        den_copy(d).wait_recv()
        den += den_recv[d - 1]
    f_row, i_row, stab_row = pick(f_gate), pick(i_gate), pick(stab_new)
    nq_row = den[0:1, 0:batch] * s_row
    kq_row = den[1:2, 0:batch] * (s_row * s_row * key_scale)
    denom = f_row * nq_row + i_row * kq_row
    bound = jnp.maximum(jnp.abs(denom), jnp.exp(-stab_row))
    mem_weight = to_col(f_row * s_row / bound)
    value_weight = to_col(i_row * kq_row / bound)
    l_wo.wait()
    numer = num_send[me].astype(jnp.float32)
    for d in range(1, n):
        for g in range(groups):
            num_copy(d, g).wait_recv()
        numer += num_recv[d - 1].astype(jnp.float32)
    numer = numer.reshape(batch, width)
    readout = mem_weight * numer + value_weight * value.astype(jnp.float32)
    hidden = (gate * readout).astype(jnp.bfloat16)

    def project(p):
        return jnp.concatenate(
            [dot(hidden, wo[:, pl.ds(pl.multiple_of(p * width + e * half, half), half)]) for e in range(cuts)], axis=1
        )

    for k in range(n - 1):
        out_send[k] = project(other(k)).astype(jnp.bfloat16)
        out_copy(k, me, other(k)).start()
    branch = project(me)
    for d in far_first:
        val_copy(d, source(d)).wait_recv()
    for p in range(n):
        val_rows[:, :, p * width : (p + 1) * width] = vals[p].astype(jnp.float32).reshape(groups, GROUP, width)

    def update_group(g, carry):
        for j in range(GROUP):
            b = g * GROUP + j
            for h in range(heads):
                at = slice(h * rows, (h + 1) * rows)
                fg = jnp.broadcast_to(f_rows[h, g, j : j + 1, :], (rows, LANES)).astype(jnp.bfloat16)
                ik = jnp.broadcast_to(kcols[g, at, j : j + 1], (rows, LANES)).astype(jnp.bfloat16)
                for c in range(0, dv, LANES):
                    val = val_rows[g, j : j + 1, h * dv + c : h * dv + c + LANES]
                    val = jnp.broadcast_to(val, (rows, LANES)).astype(jnp.bfloat16)
                    mem_out[b, at, c : c + LANES] = fg * mem[b, at, c : c + LANES] + ik * val
        return carry

    lax.fori_loop(0, groups, update_group, 0)
    for d in range(1, n):
        owner = source(d)
        out_copy(0, owner, owner).wait_recv()
        branch += out_recv[owner].astype(jnp.float32)
    res_out[...] = res[...] + branch

    for d in range(1, n):
        x_copy(d, me).wait_send()
        sq_copy(d, me).wait_send()
        val_copy(d, me).wait_send()
        den_copy(d).wait_send()
        out_copy(d - 1, me, me).wait_send()
        for g in range(groups):
            num_copy(d, g).wait_send()


def write_back(res, mem, nrm, stab, res_out, mem_out, nrm_out, stab_out, sem):
    step = mem.shape[0] // PIECES
    pairs = [(mem.at[pl.ds(i * step, step)], mem_out.at[pl.ds(i * step, step)]) for i in range(PIECES)]
    pairs += [(res, res_out), (nrm, nrm_out), (stab, stab_out)]
    copies = [pltpu.make_async_copy(a, b, sem.at[i]) for i, (a, b) in enumerate(pairs)]
    for copy in copies:
        copy.start()
    for copy in copies:
        copy.wait()


def body(
    residual, norm_gain, w_query, w_key, w_value, w_gate, w_input, w_forget, b_input, b_forget, w_out, memory, normalizer, stabilizer
):
    n = lax.axis_size("head")
    batch, width = residual.shape
    heads, rows, d_model = w_query.shape
    dv = memory.shape[3]
    hr = heads * rows
    groups = batch // GROUP
    f32, bf16 = jnp.float32, jnp.bfloat16
    args = (
        residual,
        norm_gain.reshape(1, d_model),
        w_query.reshape(hr, d_model),
        w_key.reshape(hr, d_model),
        w_value,
        w_gate,
        w_input,
        w_forget,
        b_input.reshape(1, heads),
        b_forget.reshape(1, heads),
        w_out,
        memory.reshape(batch, hr, dv),
        normalizer,
        stabilizer.T,
    )
    args = tuple(pltpu.with_memory_space_constraint(a, pltpu.HBM) for a in args)
    local = [pltpu.VMEM(a.shape, a.dtype) for a in args]
    local[1] = pltpu.VMEM((1, width), f32)
    dma = pltpu.SemaphoreType.DMA
    scratch = local + [
        pltpu.VMEM((n, batch, width), bf16),
        pltpu.VMEM((n, 1, LANES), f32),
        pltpu.VMEM((n, groups, GROUP, width), bf16),
        pltpu.VMEM((n - 1, groups, GROUP, width), bf16),
        pltpu.VMEM((heads, 2, LANES), f32),
        pltpu.VMEM((n - 1, 2, LANES), f32),
        pltpu.VMEM((n, batch, width), bf16),
        pltpu.VMEM((n - 1, batch, width), bf16),
        pltpu.VMEM((n, batch, width), bf16),
        pltpu.VMEM((hr, batch), f32),
        pltpu.VMEM((batch, hr), f32),
        pltpu.VMEM((heads, GROUP, dv), f32),
        pltpu.VMEM((groups, GROUP, n * width), f32),
        pltpu.VMEM((heads, groups, GROUP, LANES), f32),
        pltpu.VMEM((groups, hr, GROUP), f32),
        dma((13,)),
        dma((groups,)),
        dma((n - 1,)), dma((n - 1,)),
        dma((n - 1,)), dma((n - 1,)),
        dma((n - 1, groups)), dma((n - 1, groups)),
        dma((n - 1,)), dma((n - 1,)),
        dma((n - 1,)), dma((n - 1,)),
        dma((n - 1,)), dma((n,)),
    ]
    res_out, mem_out, nrm_out, stab_out = pl.pallas_call(
        functools.partial(kernel, n, batch, heads, rows, dv, width, 1.0 / math.sqrt(rows * n)),
        out_shape=(
            pltpu.VMEM((batch, width), f32),
            pltpu.VMEM((batch, hr, dv), bf16),
            pltpu.VMEM(normalizer.shape, f32),
            pltpu.VMEM((heads, batch), f32),
        ),
        in_specs=[pl.BlockSpec(memory_space=pltpu.HBM)] * len(args),
        out_specs=(pl.BlockSpec(memory_space=pltpu.VMEM),) * 4,
        scratch_shapes=scratch,
        compiler_params=pltpu.CompilerParams(collective_id=0, has_side_effects=True, vmem_limit_bytes=40 * 1024 * 1024),
        name="mlstm_step",
    )(*args)
    results = (res_out, mem_out, nrm_out, stab_out)
    res_out, mem_out, nrm_out, stab_out = pl.pallas_call(
        write_back,
        out_shape=tuple(jax.ShapeDtypeStruct(a.shape, a.dtype) for a in results),
        in_specs=[pl.BlockSpec(memory_space=pltpu.VMEM)] * 4,
        out_specs=(pl.BlockSpec(memory_space=pltpu.HBM),) * 4,
        scratch_shapes=[dma((3 + PIECES,))],
        compiler_params=pltpu.CompilerParams(vmem_limit_bytes=1024 * 1024),
        name="write_back",
    )(*(pltpu.with_memory_space_constraint(a, pltpu.VMEM) for a in results))
    return res_out, mem_out.reshape(memory.shape), nrm_out, stab_out.T


def solution(mesh):
    in_specs = (
        P("dp", "head"),
        P(),
        P(None, "head", None),
        P(None, "head", None),
        P(None, "head"),
        P(None, "head"),
        P(),
        P(),
        P(),
        P(),
        P("head", None),
        P("dp", None, "head", None),
        P("dp", None, "head"),
        P("dp", None),
    )
    out_specs = (P("dp", "head"), P("dp", None, "head", None), P("dp", None, "head"), P("dp", None))
    return jax.shard_map(body, mesh=mesh, in_specs=in_specs, out_specs=out_specs, check_vma=False)
```

```python
import functools
import math

import jax
import jax.numpy as jnp
from jax import lax
from jax.experimental import pallas as pl
from jax.experimental.pallas import tpu as pltpu
from jax.sharding import PartitionSpec as P

GROUP = 8
LANES = 128
STEP = 8
EARLY = 2
SUMMED = 2
epsilon = 1e-06

NT = (((1,), (1,)), ((), ()))
NN = (((1,), (0,)), ((), ()))


def dot(a, b, dims=NN, precision=None):
    return lax.dot_general(a, b, dims, precision=precision, preferred_element_type=jnp.float32)


def spread_values(vals, val_rows):
    n, batch, width = vals.shape
    for p in range(n):
        val_rows[p] = vals[p].astype(jnp.float32).reshape(batch // GROUP, GROUP, width)


def update_group(mem, mem_out, val_rows, f_rows, kcols, g):
    n, width = val_rows.shape[0], val_rows.shape[3]
    rows, dv = mem.shape[1] // f_rows.shape[0], mem.shape[2]

    def step(i, carry):
        for t in range(STEP):
            j = t
            b = g * GROUP + i * STEP + t
            for p in range(n):
                h, base = p * width // dv, p * width % dv
                at = slice(h * rows, (h + 1) * rows)
                fg = jnp.broadcast_to(f_rows[h, g, j : j + 1, :], (rows, LANES)).astype(jnp.bfloat16)
                ik = jnp.broadcast_to(kcols[g, at, j : j + 1], (rows, LANES)).astype(jnp.bfloat16)
                for c in range(0, width, LANES):
                    val = jnp.broadcast_to(val_rows[p, g, j : j + 1, c : c + LANES], (rows, LANES)).astype(jnp.bfloat16)
                    cols = slice(base + c, base + c + LANES)
                    mem_out[b, at, cols] = fg * mem[b, at, cols] + ik * val
        return carry

    lax.fori_loop(0, GROUP // STEP, step, 0)


def kernel(
    n, batch, heads, rows, dv, width, key_scale,
    res_hbm, gain_hbm, wq_hbm, wk_hbm, wv_hbm, wg_hbm, wi_hbm, wf_hbm, bi_hbm, bf_hbm, wo_hbm, mem_hbm, nrm_hbm, stab_hbm,
    res_out, mem, nrm_out, stab_out, vals, kcols, f_rows,
    res, gain, wq, wk, wv, wg, wi, wf, bi, bf, wo, nrm, stab,
    xs, sq, num_send, num_recv, den_send, den_recv, out_send, out_recv,
    kt_ref, qt_ref, n_rows, num_tile, val_rows,
    in_sem, mem_sem, x_send, x_recv, sq_send, sq_recv, num_ss, num_rs, den_ss, den_rs, val_ss, val_rs, out_ss, out_rs,
):
    me = lax.axis_index("head")
    groups = batch // GROUP
    hr = heads * rows
    share = n * width // heads
    barrier = pltpu.get_barrier_semaphore()

    def peer(d):
        other = me
        for k in range(n.bit_length() - 1):
            if d >> k & 1:
                other += (1 << k) * (1 - 2 * lax.rem(lax.div(me, 1 << k), 2))
        return other

    source = peer

    def other(k):
        return k + lax.div(k + n - me, n)

    far_first = sorted(range(1, n), key=lambda d: (-(d >> 1).bit_count(), d % 2))

    near = [d for d in far_first if d % 2 == 0] + [1]
    far = [d for d in far_first if d % 2 and d > 1]

    for d in far_first:
        pl.semaphore_signal(barrier, inc=1, device_id={"head": peer(d)}, device_id_type=pl.DeviceIdType.MESH)

    gain_part = gain_hbm.at[:, pl.ds(pl.multiple_of(me * width, width), width)]
    local = [
        (res_hbm, res), (gain_part, gain), (wq_hbm, wq), (wk_hbm, wk), (wi_hbm, wi), (wf_hbm, wf), (bi_hbm, bi), (bf_hbm, bf),
        (nrm_hbm, nrm), (stab_hbm, stab), (wv_hbm, wv), (wg_hbm, wg), (wo_hbm, wo),
    ]
    loads = [pltpu.make_async_copy(a, b, in_sem.at[i]) for i, (a, b) in enumerate(local)]
    (l_res, l_gain, l_wq, l_wk, l_wi, l_wf, l_bi, l_bf, l_nrm, l_stab, l_wv, l_wg, l_wo) = loads

    def mem_load(g):
        return pltpu.make_async_copy(
            mem_hbm.at[pl.ds(g * GROUP, GROUP)], mem.at[pl.ds(g * GROUP, GROUP)], mem_sem.at[g]
        )

    for copy in (l_res, l_gain, l_wq, l_wk):
        copy.start()
    for g in range(groups):
        mem_load(g).start()
    for copy in (l_wi, l_wf, l_bi, l_bf, l_nrm, l_stab, l_wv, l_wg, l_wo):
        copy.start()

    def remote(src, dst, ssem, rsem, target):
        return pltpu.make_async_remote_copy(
            src_ref=src, dst_ref=dst, send_sem=ssem, recv_sem=rsem,
            device_id={"head": target}, device_id_type=pl.DeviceIdType.MESH,
        )

    eye = lax.broadcasted_iota(jnp.int32, (batch, batch), 0) == lax.broadcasted_iota(jnp.int32, (batch, batch), 1)

    def to_row(col):
        return jnp.sum(jnp.where(eye, col, 0.0), axis=0, keepdims=True)

    def to_col(row):
        return jnp.sum(jnp.where(eye, row, 0.0), axis=1, keepdims=True)

    l_res.wait()
    l_gain.wait()
    own = res[...]
    xs[me] = (own * gain[...]).astype(jnp.bfloat16)
    sq[me] = jnp.zeros((1, LANES), jnp.float32)
    sq[me, :, 0:batch] = to_row(jnp.sum(own * own, axis=1, keepdims=True))
    den_send[...] = jnp.zeros_like(den_send)

    def x_copy(d, owner):
        return remote(xs.at[owner], xs.at[owner], x_send, x_recv.at[d - 1], peer(d))

    def sq_copy(d, owner):
        return remote(sq.at[owner], sq.at[owner], sq_send, sq_recv, peer(d))

    def val_copy(d, owner):
        return remote(vals.at[owner], vals.at[owner], val_ss, val_rs.at[0 if d == 1 else 1 + d % 2], peer(d))

    def val_relay(d):
        return remote(vals.at[peer(d)], vals.at[peer(d)], val_ss, val_rs.at[2], peer(1))

    def num_copy(d, g):
        return remote(num_send.at[peer(d), g], num_recv.at[d - 1, g], num_ss, num_rs, peer(d))

    def den_copy(d):
        head = lax.div(peer(d) * width, share)
        return remote(den_send.at[head], den_recv.at[d - 1], den_ss, den_rs, peer(d))

    def out_copy(k):
        target = other(k)
        return remote(out_send.at[k], out_recv.at[lax.rem(me + n - target, n) - 1], out_ss, out_rs, target)

    def whole(ref, ssem, rsem):
        return remote(ref, ref, ssem, rsem, peer(1))

    pl.semaphore_wait(barrier, n - 1)
    for d in [1, 3, 5, 7, 2, 4, 6]:
        x_copy(d, me).start()
    for d in far_first:
        sq_copy(d, me).start()

    l_wq.wait()
    l_wk.wait()
    l_nrm.wait()
    q_t = jnp.zeros((hr, batch), jnp.float32)
    k_t = jnp.zeros((hr, batch), jnp.float32)
    for d in [0, 1, 3, 5, 2, 4, 7, 6]:
        owner = source(d)
        if d:
            with jax.named_scope(f"qk{d}_wait"):
                x_copy(d, owner).wait_recv()
        cols = pl.ds(pl.multiple_of(owner * width, width), width)
        block = xs[owner]
        q_t += dot(wq[:, cols], block, NT)
        k_t += dot(wk[:, cols], block, NT)
    kt_ref[...] = k_t
    qt_ref[...] = q_t
    q_raw = jnp.transpose(q_t)

    mine = lax.broadcasted_iota(jnp.int32, (heads, hr), 1) // rows == lax.broadcasted_iota(jnp.int32, (heads, hr), 0)

    def numerators(g):
        block_q = q_raw[g * GROUP : (g + 1) * GROUP, :]
        for j in range(SUMMED, GROUP):
            spread = jnp.where(mine, block_q[j : j + 1, :], 0.0)
            high = spread.astype(jnp.bfloat16)
            low = (spread - high.astype(jnp.float32)).astype(jnp.bfloat16)
            both = dot(jnp.concatenate([high, low], axis=0), mem[g * GROUP + j])
            num_tile[:, j, :] = both[:heads] + both[heads:]
        for j in range(SUMMED):
            b = g * GROUP + j
            for h in range(heads):
                at = slice(h * rows, (h + 1) * rows)
                weight = jnp.broadcast_to(qt_ref[at, b : b + 1], (rows, LANES))
                for c in range(0, dv, LANES):
                    product = mem[b, at, c : c + LANES].astype(jnp.float32) * weight
                    num_tile[h, j : j + 1, c : c + LANES] = jnp.sum(product, axis=0, keepdims=True)
        for p in range(n):
            head, col = p * width // dv, p * width % dv
            num_send[p, g] = num_tile[head, :, col : col + width].astype(jnp.bfloat16)

    def split_sum(product):
        high = product.astype(jnp.bfloat16)
        low = (product - high.astype(jnp.float32)).astype(jnp.bfloat16)
        return dot(ones, high, NT) + dot(ones, low, NT)

    ones = mine.astype(jnp.bfloat16)
    for g in range(groups):
        mem_load(g).wait()
        numerators(g)
        if g == groups - 1:
            k_raw = jnp.transpose(kt_ref[...])
            for h in range(heads):
                n_rows[:, h * rows : (h + 1) * rows] = nrm[:, h, :]
            nq = split_sum(n_rows[...] * q_raw)
            kq = split_sum(k_raw * q_raw)
            for h in range(heads):
                den_send[h, 0:1, 0:batch] = nq[h : h + 1]
                den_send[h, 1:2, 0:batch] = kq[h : h + 1]
        for d in far_first:
            num_copy(d, g).start()
    for d in far_first:
        den_copy(d).start()
    all_sq = whole(sq.at[pl.ds(0, n - 1)], sq_send, sq_recv)
    all_sq.wait_recv()
    total = sq[0]
    for p in range(1, n):
        total += sq[p]
    s_row = lax.rsqrt(total[:, 0:batch] / (n * width) + epsilon)
    s_col = to_col(s_row)
    l_wv.wait()
    value = jnp.zeros((batch, width), jnp.float32)
    for p in range(n):
        value += dot(xs[p], wv[p * width : (p + 1) * width, :])
    value = (value * s_col).astype(jnp.bfloat16)
    vals[me] = value

    for copy in (l_wi, l_wf, l_bi, l_bf, l_stab):
        copy.wait()
    w_both = jnp.concatenate([wi[...], wf[...]], axis=0)
    pre = jnp.zeros((2 * heads, batch), jnp.float32)
    for p in range(n):
        pre += dot(w_both[:, p * width : (p + 1) * width], xs[p], NT)
    pre = pre * s_row
    eye_h = lax.broadcasted_iota(jnp.int32, (heads, heads), 0) == lax.broadcasted_iota(jnp.int32, (heads, heads), 1)
    bias_i = jnp.sum(jnp.where(eye_h, bi[...], 0.0), axis=1, keepdims=True)
    bias_f = jnp.sum(jnp.where(eye_h, bf[...], 0.0), axis=1, keepdims=True)
    input_pre = pre[:heads] + bias_i
    forget_pre = pre[heads:] + bias_f
    log_forget = jnp.minimum(forget_pre, 0.0) - jnp.log1p(jnp.exp(-jnp.abs(forget_pre)))
    carried = log_forget + stab[...]
    stab_new = jnp.maximum(carried, input_pre)
    stab_out[...] = stab_new
    i_gate = jnp.exp(input_pre - stab_new)
    f_gate = jnp.exp(carried - stab_new)

    key = k_raw * (s_col * key_scale)
    l_wg.wait()
    cuts = 2 if width % (2 * LANES) == 0 else 1
    half = width // cuts
    gates2 = [jnp.zeros((batch, half), jnp.float32) for _ in range(cuts)]
    for p in range(n):
        for e in range(cuts):
            gates2[e] += dot(xs[p], wg[p * width : (p + 1) * width, e * half : (e + 1) * half])
    gate = jnp.concatenate(gates2, axis=1)
    gate = jax.nn.sigmoid(gate * s_col)
    for d in near:
        val_copy(d, me).start()

    key_t = kt_ref[...] * (s_row * key_scale)
    for h in range(heads):
        at = slice(h * rows, (h + 1) * rows)
        ik = key_t[at, :] * i_gate[h : h + 1, :]
        f_rows[h] = jnp.broadcast_to(to_col(f_gate[h : h + 1, :]), (batch, LANES)).reshape(groups, GROUP, LANES)
        for g in range(groups):
            kcols[g, at, :] = ik[:, g * GROUP : (g + 1) * GROUP]
    for h in range(heads):
        nrm_out[:, h, :] = to_col(f_gate[h : h + 1, :]) * nrm[:, h, :] + (
            to_col(i_gate[h : h + 1, :]) * key[:, h * rows : (h + 1) * rows]
        )

    my_head = lax.div(me * width, share)
    picked = lax.broadcasted_iota(jnp.int32, (heads, batch), 0) == my_head

    def pick(table):
        return jnp.sum(jnp.where(picked, table, 0.0), axis=0, keepdims=True)

    den = den_send[my_head]
    all_den = whole(den_recv, den_ss, den_rs)
    all_den.wait_recv()
    for d in range(1, n):
        den += den_recv[d - 1]
    f_row, i_row, stab_row = pick(f_gate), pick(i_gate), pick(stab_new)
    nq_row = den[0:1, 0:batch] * s_row
    kq_row = den[1:2, 0:batch] * (s_row * s_row * key_scale)
    denom = f_row * nq_row + i_row * kq_row
    bound = jnp.maximum(jnp.abs(denom), jnp.exp(-stab_row))
    mem_weight = to_col(f_row * s_row / bound)
    value_weight = to_col(i_row * kq_row / bound)
    l_wo.wait()
    numer = num_send[me].astype(jnp.float32)
    all_num = whole(num_recv, num_ss, num_rs)
    all_num.wait_recv()
    for d in range(1, n):
        numer += num_recv[d - 1].astype(jnp.float32)
    numer = numer.reshape(batch, width)
    readout = mem_weight * numer + value_weight * value.astype(jnp.float32)
    hidden = (gate * readout).astype(jnp.bfloat16)

    def project(p):
        return jnp.concatenate(
            [dot(hidden, wo[:, pl.ds(pl.multiple_of(p * width + e * half, half), half)]) for e in range(cuts)], axis=1
        )

    out_send[0] = project(other(0)).astype(jnp.bfloat16)
    out_copy(0).start()
    for k in range(1, n, 2):
        for c in range(k, min(k + 2, n - 1)):
            out_send[c] = project(other(c)).astype(jnp.bfloat16)
        if k + 1 >= n - 1:
            branch = project(me)
        for c in range(k, min(k + 2, n - 1)):
            out_copy(c).start()
    if n > 2:
        whole(vals.at[pl.ds(0, n // 2 - 1)], val_ss, val_rs.at[1]).wait_recv()
    for d in near[:-1]:
        val_relay(d).start()
    val_copy(1, source(1)).wait_recv()
    if n > 2:
        whole(vals.at[pl.ds(0, n // 2 - 1)], val_ss, val_rs.at[2]).wait_recv()
    spread_values(vals, val_rows)
    for g in range(EARLY):
        update_group(mem, mem, val_rows, f_rows, kcols, g)
    all_out = whole(out_recv, out_ss, out_rs)
    all_out.wait_recv()
    for d in range(1, n):
        branch += out_recv[d - 1].astype(jnp.float32)
    res_out[...] = res[...] + branch

    whole(xs.at[pl.ds(0, n - 1)], x_send, x_recv.at[0]).wait_send()
    whole(vals.at[pl.ds(0, n - 1)], val_ss, val_rs.at[0]).wait_send()
    for copy in (all_sq, all_num, all_den, all_out):
        copy.wait_send()

def write_back(res, mem, nrm, stab, vals, kcols, f_rows, res_out, mem_out, nrm_out, stab_out, staged, val_rows, sem):
    groups = mem.shape[0] // GROUP

    def block(g, source):
        part = pl.ds(g * GROUP, GROUP)
        return pltpu.make_async_copy(source.at[part], mem_out.at[part], sem.at[g])

    copies = [block(g, mem) for g in range(EARLY)]
    copies += [
        pltpu.make_async_copy(a, b, sem.at[groups + i])
        for i, (a, b) in enumerate([(res, res_out), (nrm, nrm_out), (stab, stab_out)])
    ]
    for copy in copies:
        copy.start()
    spread_values(vals, val_rows)
    for g in range(EARLY, groups):
        update_group(mem, staged, val_rows, f_rows, kcols, g)
        copies.append(block(g, staged))
        copies[-1].start()
    for copy in copies:
        copy.wait()


def body(
    residual, norm_gain, w_query, w_key, w_value, w_gate, w_input, w_forget, b_input, b_forget, w_out, memory, normalizer, stabilizer
):
    n = lax.axis_size("head")
    batch, width = residual.shape
    heads, rows, d_model = w_query.shape
    dv = memory.shape[3]
    hr = heads * rows
    groups = batch // GROUP
    f32, bf16 = jnp.float32, jnp.bfloat16
    args = (
        residual,
        norm_gain.reshape(1, d_model),
        w_query.reshape(hr, d_model),
        w_key.reshape(hr, d_model),
        w_value,
        w_gate,
        w_input,
        w_forget,
        b_input.reshape(1, heads),
        b_forget.reshape(1, heads),
        w_out,
        memory.reshape(batch, hr, dv),
        normalizer,
        stabilizer.T,
    )
    args = tuple(pltpu.with_memory_space_constraint(a, pltpu.HBM) for a in args)
    local = [pltpu.VMEM(a.shape, a.dtype) for a in args]
    local[1] = pltpu.VMEM((1, width), f32)
    del local[11]
    dma = pltpu.SemaphoreType.DMA
    scratch = local + [
        pltpu.VMEM((n, batch, width), bf16),
        pltpu.VMEM((n, 1, LANES), f32),
        pltpu.VMEM((n, groups, GROUP, width), bf16),
        pltpu.VMEM((n - 1, groups, GROUP, width), bf16),
        pltpu.VMEM((heads, 2, LANES), f32),
        pltpu.VMEM((n - 1, 2, LANES), f32),
        pltpu.VMEM((n - 1, batch, width), bf16),
        pltpu.VMEM((n - 1, batch, width), bf16),
        pltpu.VMEM((hr, batch), f32),
        pltpu.VMEM((hr, batch), f32),
        pltpu.VMEM((batch, hr), f32),
        pltpu.VMEM((heads, GROUP, dv), f32),
        pltpu.VMEM((n, groups, GROUP, width), f32),
        dma((13,)),
        dma((groups,)),
        dma, dma((n - 1,)),
        dma, dma, dma, dma, dma, dma,
        dma, dma((3,)),
        dma, dma,
    ]
    results = pl.pallas_call(
        functools.partial(kernel, n, batch, heads, rows, dv, width, 1.0 / math.sqrt(rows * n)),
        out_shape=(
            pltpu.VMEM((batch, width), f32),
            pltpu.VMEM((batch, hr, dv), bf16),
            pltpu.VMEM(normalizer.shape, f32),
            pltpu.VMEM((heads, batch), f32),
            pltpu.VMEM((n, batch, width), bf16),
            pltpu.VMEM((groups, hr, GROUP), f32),
            pltpu.VMEM((heads, groups, GROUP, LANES), f32),
        ),
        in_specs=[pl.BlockSpec(memory_space=pltpu.HBM)] * len(args),
        out_specs=(pl.BlockSpec(memory_space=pltpu.VMEM),) * 7,
        scratch_shapes=scratch,
        compiler_params=pltpu.CompilerParams(collective_id=0, has_side_effects=True, vmem_limit_bytes=40 * 1024 * 1024),
        name="mlstm_step",
    )(*args)
    res_out, mem_out, nrm_out, stab_out = pl.pallas_call(
        write_back,
        out_shape=tuple(jax.ShapeDtypeStruct(a.shape, a.dtype) for a in results[:4]),
        in_specs=[pl.BlockSpec(memory_space=pltpu.VMEM)] * 7,
        out_specs=(pl.BlockSpec(memory_space=pltpu.HBM),) * 4,
        scratch_shapes=[
            pltpu.VMEM((batch, hr, dv), bf16),
            pltpu.VMEM((n, groups, GROUP, width), f32),
            dma((3 + groups,)),
        ],
        compiler_params=pltpu.CompilerParams(vmem_limit_bytes=12 * 1024 * 1024),
        name="write_back",
    )(*(pltpu.with_memory_space_constraint(a, pltpu.VMEM) for a in results))
    return res_out, mem_out.reshape(memory.shape), nrm_out, stab_out.T


def solution(mesh):
    in_specs = (
        P("dp", "head"),
        P(),
        P(None, "head", None),
        P(None, "head", None),
        P(None, "head"),
        P(None, "head"),
        P(),
        P(),
        P(),
        P(),
        P("head", None),
        P("dp", None, "head", None),
        P("dp", None, "head"),
        P("dp", None),
    )
    out_specs = (P("dp", "head"), P("dp", None, "head", None), P("dp", None, "head"), P("dp", None))
    return jax.shard_map(body, mesh=mesh, in_specs=in_specs, out_specs=out_specs, check_vma=False)
```

```python
import functools
import math

import jax
import jax.numpy as jnp
from jax import lax
from jax.experimental import pallas as pl
from jax.experimental.pallas import tpu as pltpu
from jax.sharding import PartitionSpec as P

GROUP = 8
LANES = 128
STEP = 8
EARLY = 2
SUMMED = 2
epsilon = 1e-06

NT = (((1,), (1,)), ((), ()))
NN = (((1,), (0,)), ((), ()))


def dot(a, b, dims=NN, precision=None):
    return lax.dot_general(a, b, dims, precision=precision, preferred_element_type=jnp.float32)


def spread_values(vals, val_rows):
    n, batch, width = vals.shape
    for p in range(n):
        val_rows[p] = vals[p].astype(jnp.float32).reshape(batch // GROUP, GROUP, width)


def update_group(mem, mem_out, val_rows, f_rows, kcols, g):
    n, width = val_rows.shape[0], val_rows.shape[3]
    rows, dv = mem.shape[1] // f_rows.shape[0], mem.shape[2]

    def step(i, carry):
        for t in range(STEP):
            j = t
            b = g * GROUP + i * STEP + t
            for p in range(n):
                h, base = p * width // dv, p * width % dv
                at = slice(h * rows, (h + 1) * rows)
                fg = jnp.broadcast_to(f_rows[h, g, j : j + 1, :], (rows, LANES)).astype(jnp.bfloat16)
                ik = jnp.broadcast_to(kcols[g, at, j : j + 1], (rows, LANES)).astype(jnp.bfloat16)
                for c in range(0, width, LANES):
                    val = jnp.broadcast_to(val_rows[p, g, j : j + 1, c : c + LANES], (rows, LANES)).astype(jnp.bfloat16)
                    cols = slice(base + c, base + c + LANES)
                    mem_out[b, at, cols] = fg * mem[b, at, cols] + ik * val
        return carry

    lax.fori_loop(0, GROUP // STEP, step, 0)


def kernel(
    n, batch, heads, rows, dv, width, key_scale,
    res_hbm, gain_hbm, wq_hbm, wk_hbm, wv_hbm, wg_hbm, wi_hbm, wf_hbm, bi_hbm, bf_hbm, wo_hbm, mem_hbm, nrm_hbm, stab_hbm,
    res_out, mem, nrm_out, stab_out, vals, kcols, f_rows,
    res, gain, wq, wk, wv, wg, wi, wf, bi, bf, wo, nrm, stab,
    xs, sq, num_send, num_recv, den_send, den_recv, out_send, out_recv,
    kt_ref, qt_ref, n_rows, num_tile, val_rows,
    in_sem, mem_sem, wide_ss, x_recv, sq_send, sq_recv, num_rs, den_ss, den_rs, val_rs, out_rs,
):
    me = lax.axis_index("head")
    groups = batch // GROUP
    hr = heads * rows
    share = n * width // heads
    barrier = pltpu.get_barrier_semaphore()

    def peer(d):
        other = me
        for k in range(n.bit_length() - 1):
            if d >> k & 1:
                other += (1 << k) * (1 - 2 * lax.rem(lax.div(me, 1 << k), 2))
        return other

    source = peer

    def other(k):
        return n - k - lax.div(me + k, n) if k else lax.div(n - me, n)

    far_first = sorted(range(1, n), key=lambda d: (-(d >> 1).bit_count(), 1 - d % 2, d))

    near = [d for d in far_first if d % 2 == 0] + [1]
    far = [d for d in far_first if d % 2 and d > 1]

    for d in far_first:
        pl.semaphore_signal(barrier, inc=1, device_id={"head": peer(d)}, device_id_type=pl.DeviceIdType.MESH)

    gain_part = gain_hbm.at[:, pl.ds(pl.multiple_of(me * width, width), width)]
    local = [
        (res_hbm, res), (gain_part, gain), (wq_hbm, wq), (wk_hbm, wk), (wi_hbm, wi), (wf_hbm, wf), (bi_hbm, bi), (bf_hbm, bf),
        (nrm_hbm, nrm), (stab_hbm, stab), (wv_hbm, wv), (wg_hbm, wg), (wo_hbm, wo),
    ]
    loads = [pltpu.make_async_copy(a, b, in_sem.at[i]) for i, (a, b) in enumerate(local)]
    (l_res, l_gain, l_wq, l_wk, l_wi, l_wf, l_bi, l_bf, l_nrm, l_stab, l_wv, l_wg, l_wo) = loads

    def mem_load(g):
        return pltpu.make_async_copy(
            mem_hbm.at[pl.ds(g * GROUP, GROUP)], mem.at[pl.ds(g * GROUP, GROUP)], mem_sem.at[g]
        )

    for copy in (l_res, l_gain, l_wq, l_wk):
        copy.start()
    for g in range(groups):
        mem_load(g).start()
    for copy in (l_wi, l_wf, l_bi, l_bf, l_nrm, l_stab, l_wv, l_wg, l_wo):
        copy.start()

    def remote(src, dst, ssem, rsem, target):
        return pltpu.make_async_remote_copy(
            src_ref=src, dst_ref=dst, send_sem=ssem, recv_sem=rsem,
            device_id={"head": target}, device_id_type=pl.DeviceIdType.MESH,
        )

    eye = lax.broadcasted_iota(jnp.int32, (batch, batch), 0) == lax.broadcasted_iota(jnp.int32, (batch, batch), 1)

    def to_row(col):
        return jnp.sum(jnp.where(eye, col, 0.0), axis=0, keepdims=True)

    def to_col(row):
        return jnp.sum(jnp.where(eye, row, 0.0), axis=1, keepdims=True)

    l_res.wait()
    l_gain.wait()
    own = res[...]
    xs[me] = (own * gain[...]).astype(jnp.bfloat16)
    sq[me] = jnp.zeros((1, LANES), jnp.float32)
    sq[me, :, 0:batch] = to_row(jnp.sum(own * own, axis=1, keepdims=True))
    den_send[...] = jnp.zeros_like(den_send)

    def x_copy(d, owner):
        return remote(xs.at[owner], xs.at[owner], wide_ss, x_recv.at[d - 1], peer(d))

    def sq_copy(d, owner):
        return remote(sq.at[owner], sq.at[owner], sq_send, sq_recv, peer(d))

    def val_copy(d, owner):
        return remote(vals.at[owner], vals.at[owner], wide_ss, val_rs.at[0 if d == 1 else 1 + d % 2], peer(d))

    def val_relay(d):
        return remote(vals.at[peer(d)], vals.at[peer(d)], wide_ss, val_rs.at[2], peer(1))

    def num_copy(d, g):
        return remote(num_send.at[peer(d), g], num_recv.at[d - 1, g], wide_ss, num_rs, peer(d))

    def den_copy(d):
        head = lax.div(peer(d) * width, share)
        return remote(den_send.at[head], den_recv.at[d - 1], den_ss, den_rs, peer(d))

    def out_copy(k):
        target = other(k)
        return remote(out_send.at[k], out_recv.at[lax.rem(me + n - target, n) - 1], wide_ss, out_rs, target)

    def whole(ref, ssem, rsem):
        return remote(ref, ref, ssem, rsem, peer(1))

    pl.semaphore_wait(barrier, n - 1)
    for d in sorted(range(1, n), key=lambda d: (1 - d % 2, d)):
        x_copy(d, me).start()
    for d in far_first:
        sq_copy(d, me).start()

    l_wq.wait()
    l_wk.wait()
    l_nrm.wait()
    q_t = jnp.zeros((hr, batch), jnp.float32)
    k_t = jnp.zeros((hr, batch), jnp.float32)
    for d in sorted(range(n), key=lambda d: ((d >> 1).bit_count(), d > 0, 1 - d % 2, d)):
        owner = source(d)
        if d:
            x_copy(d, owner).wait_recv()
        cols = pl.ds(pl.multiple_of(owner * width, width), width)
        block = xs[owner]
        q_t += dot(wq[:, cols], block, NT)
        k_t += dot(wk[:, cols], block, NT)
    kt_ref[...] = k_t
    qt_ref[...] = q_t
    q_raw = jnp.transpose(q_t)

    mine = lax.broadcasted_iota(jnp.int32, (heads, hr), 1) // rows == lax.broadcasted_iota(jnp.int32, (heads, hr), 0)

    def numerators(g):
        block_q = q_raw[g * GROUP : (g + 1) * GROUP, :]
        for j in range(SUMMED, GROUP):
            spread = jnp.where(mine, block_q[j : j + 1, :], 0.0)
            high = spread.astype(jnp.bfloat16)
            low = (spread - high.astype(jnp.float32)).astype(jnp.bfloat16)
            both = dot(jnp.concatenate([high, low], axis=0), mem[g * GROUP + j])
            num_tile[:, j, :] = both[:heads] + both[heads:]
        for j in range(SUMMED):
            b = g * GROUP + j
            for h in range(heads):
                at = slice(h * rows, (h + 1) * rows)
                weight = jnp.broadcast_to(qt_ref[at, b : b + 1], (rows, LANES))
                for c in range(0, dv, LANES):
                    product = mem[b, at, c : c + LANES].astype(jnp.float32) * weight
                    num_tile[h, j : j + 1, c : c + LANES] = jnp.sum(product, axis=0, keepdims=True)
        for p in range(n):
            head, col = p * width // dv, p * width % dv
            num_send[p, g] = num_tile[head, :, col : col + width].astype(jnp.bfloat16)

    def split_sum(product):
        high = product.astype(jnp.bfloat16)
        low = (product - high.astype(jnp.float32)).astype(jnp.bfloat16)
        return dot(ones, high, NT) + dot(ones, low, NT)

    ones = mine.astype(jnp.bfloat16)
    for g in range(groups):
        mem_load(g).wait()
        numerators(g)
        if g == groups - 1:
            k_raw = jnp.transpose(kt_ref[...])
            for h in range(heads):
                n_rows[:, h * rows : (h + 1) * rows] = nrm[:, h, :]
            nq = split_sum(n_rows[...] * q_raw)
            kq = split_sum(k_raw * q_raw)
            for h in range(heads):
                den_send[h, 0:1, 0:batch] = nq[h : h + 1]
                den_send[h, 1:2, 0:batch] = kq[h : h + 1]
        for d in far_first:
            num_copy(d, g).start()
    for d in far_first:
        den_copy(d).start()
    all_sq = whole(sq.at[pl.ds(0, n - 1)], sq_send, sq_recv)
    all_sq.wait_recv()
    total = sq[0]
    for p in range(1, n):
        total += sq[p]
    s_row = lax.rsqrt(total[:, 0:batch] / (n * width) + epsilon)
    s_col = to_col(s_row)
    l_wv.wait()
    value = jnp.zeros((batch, width), jnp.float32)
    for p in range(n):
        value += dot(xs[p], wv[p * width : (p + 1) * width, :])
    value = (value * s_col).astype(jnp.bfloat16)
    vals[me] = value

    for copy in (l_wi, l_wf, l_bi, l_bf, l_stab):
        copy.wait()
    w_both = jnp.concatenate([wi[...], wf[...]], axis=0)
    pre = jnp.zeros((2 * heads, batch), jnp.float32)
    for p in range(n):
        pre += dot(w_both[:, p * width : (p + 1) * width], xs[p], NT)
    pre = pre * s_row
    eye_h = lax.broadcasted_iota(jnp.int32, (heads, heads), 0) == lax.broadcasted_iota(jnp.int32, (heads, heads), 1)
    bias_i = jnp.sum(jnp.where(eye_h, bi[...], 0.0), axis=1, keepdims=True)
    bias_f = jnp.sum(jnp.where(eye_h, bf[...], 0.0), axis=1, keepdims=True)
    input_pre = pre[:heads] + bias_i
    forget_pre = pre[heads:] + bias_f
    log_forget = jnp.minimum(forget_pre, 0.0) - jnp.log1p(jnp.exp(-jnp.abs(forget_pre)))
    carried = log_forget + stab[...]
    stab_new = jnp.maximum(carried, input_pre)
    stab_out[...] = stab_new
    i_gate = jnp.exp(input_pre - stab_new)
    f_gate = jnp.exp(carried - stab_new)

    key = k_raw * (s_col * key_scale)
    l_wg.wait()
    cuts = 2 if width % (2 * LANES) == 0 else 1
    half = width // cuts
    gates2 = [jnp.zeros((batch, half), jnp.float32) for _ in range(cuts)]
    for p in range(n):
        for e in range(cuts):
            gates2[e] += dot(xs[p], wg[p * width : (p + 1) * width, e * half : (e + 1) * half])
    gate = jnp.concatenate(gates2, axis=1)
    gate = jax.nn.sigmoid(gate * s_col)
    for d in near:
        val_copy(d, me).start()

    my_head = lax.div(me * width, share)
    picked = lax.broadcasted_iota(jnp.int32, (heads, batch), 0) == my_head

    def pick(table):
        return jnp.sum(jnp.where(picked, table, 0.0), axis=0, keepdims=True)

    den = den_send[my_head]
    all_den = whole(den_recv, den_ss, den_rs)
    all_den.wait_recv()
    for d in range(1, n):
        den += den_recv[d - 1]
    f_row, i_row, stab_row = pick(f_gate), pick(i_gate), pick(stab_new)
    nq_row = den[0:1, 0:batch] * s_row
    kq_row = den[1:2, 0:batch] * (s_row * s_row * key_scale)
    denom = f_row * nq_row + i_row * kq_row
    bound = jnp.maximum(jnp.abs(denom), jnp.exp(-stab_row))
    mem_weight = to_col(f_row * s_row / bound)
    value_weight = to_col(i_row * kq_row / bound)
    l_wo.wait()
    numer = num_send[me].astype(jnp.float32)
    all_num = whole(num_recv, wide_ss, num_rs)
    all_num.wait_recv()
    for d in range(1, n):
        numer += num_recv[d - 1].astype(jnp.float32)
    numer = numer.reshape(batch, width)
    readout = mem_weight * numer + value_weight * value.astype(jnp.float32)
    hidden = (gate * readout).astype(jnp.bfloat16)

    def project(p):
        return jnp.concatenate(
            [dot(hidden, wo[:, pl.ds(pl.multiple_of(p * width + e * half, half), half)]) for e in range(cuts)], axis=1
        )

    out_send[0] = project(other(0)).astype(jnp.bfloat16)
    out_copy(0).start()
    for k in range(1, n, 2):
        for c in range(k, min(k + 2, n - 1)):
            out_send[c] = project(other(c)).astype(jnp.bfloat16)
        if k + 1 >= n - 1:
            branch = project(me)
        for c in range(k, min(k + 2, n - 1)):
            out_copy(c).start()
    if n > 2:
        whole(vals.at[pl.ds(0, n // 2 - 1)], wide_ss, val_rs.at[1]).wait_recv()
    for d in near[:-1]:
        val_relay(d).start()
    key_t = kt_ref[...] * (s_row * key_scale)
    for h in range(heads):
        at = slice(h * rows, (h + 1) * rows)
        ik = key_t[at, :] * i_gate[h : h + 1, :]
        f_rows[h] = jnp.broadcast_to(to_col(f_gate[h : h + 1, :]), (batch, LANES)).reshape(groups, GROUP, LANES)
        for g in range(groups):
            kcols[g, at, :] = ik[:, g * GROUP : (g + 1) * GROUP]
    for h in range(heads):
        nrm_out[:, h, :] = to_col(f_gate[h : h + 1, :]) * nrm[:, h, :] + (
            to_col(i_gate[h : h + 1, :]) * key[:, h * rows : (h + 1) * rows]
        )

    val_copy(1, source(1)).wait_recv()
    if n > 2:
        whole(vals.at[pl.ds(0, n // 2 - 1)], wide_ss, val_rs.at[2]).wait_recv()
    spread_values(vals, val_rows)
    for g in range(EARLY):
        update_group(mem, mem, val_rows, f_rows, kcols, g)
    all_out = whole(out_recv, wide_ss, out_rs)
    all_out.wait_recv()
    for d in range(1, n):
        branch += out_recv[d - 1].astype(jnp.float32)
    res_out[...] = res[...] + branch

    whole(wv.at[pl.ds(0, 4 * (n - 1) * batch)], wide_ss, out_rs).wait_send()
    all_sq.wait_send()
    all_den.wait_send()

def write_back(res, mem, nrm, stab, vals, kcols, f_rows, res_out, mem_out, nrm_out, stab_out, staged, val_rows, sem):
    groups = mem.shape[0] // GROUP

    def block(g, source):
        part = pl.ds(g * GROUP, GROUP)
        return pltpu.make_async_copy(source.at[part], mem_out.at[part], sem.at[g])

    copies = [block(g, mem) for g in range(EARLY)]
    copies += [
        pltpu.make_async_copy(a, b, sem.at[groups + i])
        for i, (a, b) in enumerate([(res, res_out), (nrm, nrm_out), (stab, stab_out)])
    ]
    for copy in copies:
        copy.start()
    spread_values(vals, val_rows)
    for g in range(EARLY, groups):
        update_group(mem, staged, val_rows, f_rows, kcols, g)
        copies.append(block(g, staged))
        copies[-1].start()
    for copy in copies:
        copy.wait()


def body(
    residual, norm_gain, w_query, w_key, w_value, w_gate, w_input, w_forget, b_input, b_forget, w_out, memory, normalizer, stabilizer
):
    n = lax.axis_size("head")
    batch, width = residual.shape
    heads, rows, d_model = w_query.shape
    dv = memory.shape[3]
    hr = heads * rows
    groups = batch // GROUP
    f32, bf16 = jnp.float32, jnp.bfloat16
    args = (
        residual,
        norm_gain.reshape(1, d_model),
        w_query.reshape(hr, d_model),
        w_key.reshape(hr, d_model),
        w_value,
        w_gate,
        w_input,
        w_forget,
        b_input.reshape(1, heads),
        b_forget.reshape(1, heads),
        w_out,
        memory.reshape(batch, hr, dv),
        normalizer,
        stabilizer.T,
    )
    args = tuple(pltpu.with_memory_space_constraint(a, pltpu.HBM) for a in args)
    local = [pltpu.VMEM(a.shape, a.dtype) for a in args]
    local[1] = pltpu.VMEM((1, width), f32)
    del local[11]
    dma = pltpu.SemaphoreType.DMA
    scratch = local + [
        pltpu.VMEM((n, batch, width), bf16),
        pltpu.VMEM((n, 1, LANES), f32),
        pltpu.VMEM((n, groups, GROUP, width), bf16),
        pltpu.VMEM((n - 1, groups, GROUP, width), bf16),
        pltpu.VMEM((heads, 2, LANES), f32),
        pltpu.VMEM((n - 1, 2, LANES), f32),
        pltpu.VMEM((n - 1, batch, width), bf16),
        pltpu.VMEM((n - 1, batch, width), bf16),
        pltpu.VMEM((hr, batch), f32),
        pltpu.VMEM((hr, batch), f32),
        pltpu.VMEM((batch, hr), f32),
        pltpu.VMEM((heads, GROUP, dv), f32),
        pltpu.VMEM((n, groups, GROUP, width), f32),
        dma((13,)),
        dma((groups,)),
        dma, dma((n - 1,)),
        dma, dma, dma, dma, dma,
        dma((3,)), dma,
    ]
    results = pl.pallas_call(
        functools.partial(kernel, n, batch, heads, rows, dv, width, 1.0 / math.sqrt(rows * n)),
        out_shape=(
            pltpu.VMEM((batch, width), f32),
            pltpu.VMEM((batch, hr, dv), bf16),
            pltpu.VMEM(normalizer.shape, f32),
            pltpu.VMEM((heads, batch), f32),
            pltpu.VMEM((n, batch, width), bf16),
            pltpu.VMEM((groups, hr, GROUP), f32),
            pltpu.VMEM((heads, groups, GROUP, LANES), f32),
        ),
        in_specs=[pl.BlockSpec(memory_space=pltpu.HBM)] * len(args),
        out_specs=(pl.BlockSpec(memory_space=pltpu.VMEM),) * 7,
        scratch_shapes=scratch,
        compiler_params=pltpu.CompilerParams(collective_id=0, has_side_effects=True, vmem_limit_bytes=40 * 1024 * 1024),
        name="mlstm_step",
    )(*args)
    res_out, mem_out, nrm_out, stab_out = pl.pallas_call(
        write_back,
        out_shape=tuple(jax.ShapeDtypeStruct(a.shape, a.dtype) for a in results[:4]),
        in_specs=[pl.BlockSpec(memory_space=pltpu.VMEM)] * 7,
        out_specs=(pl.BlockSpec(memory_space=pltpu.HBM),) * 4,
        scratch_shapes=[
            pltpu.VMEM((batch, hr, dv), bf16),
            pltpu.VMEM((n, groups, GROUP, width), f32),
            dma((3 + groups,)),
        ],
        compiler_params=pltpu.CompilerParams(vmem_limit_bytes=12 * 1024 * 1024),
        name="write_back",
    )(*(pltpu.with_memory_space_constraint(a, pltpu.VMEM) for a in results))
    return res_out, mem_out.reshape(memory.shape), nrm_out, stab_out.T


def solution(mesh):
    in_specs = (
        P("dp", "head"),
        P(),
        P(None, "head", None),
        P(None, "head", None),
        P(None, "head"),
        P(None, "head"),
        P(),
        P(),
        P(),
        P(),
        P("head", None),
        P("dp", None, "head", None),
        P("dp", None, "head"),
        P("dp", None),
    )
    out_specs = (P("dp", "head"), P("dp", None, "head", None), P("dp", None, "head"), P("dp", None))
    return jax.shard_map(body, mesh=mesh, in_specs=in_specs, out_specs=out_specs, check_vma=False)
```
